128 devices in a mesh: narrow: 4 (over y), wide: 32 (over z, x, core).
Axes of the slice: x: 4, y: 4, z: 4, core: 2. Of those that a mesh axis runs over, the one named last changes fastest.
Arguments:
- level_set: float32 [1024, 256, 512], P('wide', 'narrow')
- velocity: bfloat16 [3, 1024, 256, 512], P(None, 'wide', 'narrow'), may hold values from -2 to 2
- box_owner: int32 [32, 4, 256, 1], P('wide', 'narrow'), may hold values from 0 to 31; in each aligned block of 256 rows (0 to 255, 256 to 511, ..., all dimensions but the last counted through in order) at most 20 rows name the same one
Outputs:
- surface: float32 [1024, 256, 512], P('wide', 'narrow')
- box_fractions: float32 [32, 4, 640, 512], P('wide', 'narrow')
The draws below stay inside these ranges and needn't reach their ends.
Inputs may be any that keep to these rules, and one draw needn't show every extreme that they name: `box_owner`: the tiles of one device name one box owner at most 20 times.
All inputs are finite; a program needn't handle non-finite values.
Results may differ from the reference program's by a relative error of at most 0.0003.
Values sent between devices are 32-bit elements; how exact they have to be, the bound alone decides.
A program may use at most 192 MiB of HBM per device.

```python
import math
import jax
import jax.numpy as jnp
import numpy as np
from jax import lax

TILE = 16
CX = 32
CY = 64
CZ = 512
SWEEPS = 3
NX = 1024
NY = 256
TPD = 256
CAP = 20
N_NARROW = 4
N_WIDE = 32


def draw_level_set(key, part):
    keys = jax.random.split(key, 3)
    phases = jax.random.uniform(keys[0], (4,), jnp.float32, 0.0, 2.0 * math.pi)
    coord_x = jnp.arange(NX, dtype=jnp.float32)[:, None]
    coord_y = jnp.arange(NY, dtype=jnp.float32)[None, :]
    waves = jnp.sin(2.0 * math.pi * coord_x / NX + phases[0]) + jnp.sin(4.0 * math.pi * coord_y / NY + phases[1])
    waves = waves + 0.5 * jnp.sin(2.0 * math.pi * (coord_x / NX + coord_y / NY) * 3.0 + phases[2])
    roughness = jax.random.uniform(keys[1], (NX, NY), jnp.float32, -3.0, 3.0)
    height = CZ * 0.5 + CZ * 0.12 * waves + roughness
    noise = 0.5 * jax.random.normal(keys[2], (NX, NY, CZ), jnp.float32)
    coord_z = jnp.arange(CZ, dtype=jnp.float32)[None, None, :]
    return 4.0 * jnp.tanh((coord_z - height[:, :, None]) / 6.0) + noise


def block_scale(rng, shape, shards, low, high):
    def one(dim, blocks):
        heights = jax.random.uniform(jax.random.fold_in(jax.random.fold_in(rng, 6), dim), (blocks,), jnp.float32, low / len(shards), high / len(shards))
        return jnp.repeat(jnp.exp(heights), shape[dim] // blocks).reshape((-1,) + (1,) * (len(shape) - dim - 1))

    factor_of = one(*shards[0])
    for cut in shards[1:]:
        factor_of = factor_of * one(*cut)
    return factor_of


def shared_out(stream_key, own, number, rows, number_of, top, most, lean):
    ranking = jax.random.permutation(stream_key, number_of)
    packed, ordinary = load_shares(number_of, rows * top, most, lean, True), load_shares(number_of, rows * top, most, lean, False)
    places = jnp.arange(number_of)

    def named(tallies, rotation):
        used = int((tallies > 0).sum())
        fixed = max(1, used // 4)
        shifted = fixed + (places - fixed + rotation * (used - fixed)) % max(1, number_of - fixed)
        return jnp.zeros((number_of,), jnp.int32).at[ranking[jnp.where(places < fixed, places, shifted)]].set(jnp.asarray(tallies, jnp.int32))

    tallies = jnp.where(number % 4 == 0, named(packed, number // 4), named(ordinary, number - number // 4 - 1))
    mixed = jax.random.permutation(jax.random.fold_in(own, 3), number_of)
    source_of, sink = mixed[0:number_of // 2 * 2:2], mixed[1:number_of // 2 * 2:2]
    margin = jnp.minimum(tallies[source_of] - 1, most - tallies[sink]) // 2
    margin = jnp.where((source_of == ranking[0]) | (sink == ranking[0]) | (tallies[sink] == 0), 0, jnp.maximum(margin, 0))
    shifted = jax.random.randint(jax.random.fold_in(own, 4), (number_of // 2,), 0, 1 << 20) % (margin + 1)
    tallies = tallies.at[source_of].add(-shifted).at[sink].add(shifted)
    items = jnp.searchsorted(jnp.cumsum(tallies), jnp.arange(rows * top), side="right").astype(jnp.int32)
    grid = items.reshape(top, rows).T
    grid = grid[jax.random.permutation(jax.random.fold_in(own, 1), rows)]
    rotation = jax.random.randint(jax.random.fold_in(own, 2), (rows, 1), 0, top)
    return jnp.take_along_axis(grid, (jnp.arange(top)[None, :] + rotation) % top, axis=1)


def load_shares(count, total, limit, skew, full):
    loads = [(1 << 20) // math.isqrt(rank ** skew) + 1 for rank in range(1, count + 1)]
    largest = limit if full else min(limit, max(-(-total // count), total * loads[0] // sum(loads)))
    least = 1 if total - largest >= count - 1 else 0
    given, surplus = [largest] + [least] * (count - 1), total - largest - least * (count - 1)
    while surplus > 0:
        candidates = [i for i in range(1, count) if given[i] < largest] or [i for i in range(1, count) if given[i] < limit]
        whole, budget = sum([loads[i] for i in candidates]), surplus
        for i in candidates:
            more = min(limit - given[i], max(1, budget * loads[i] // whole), surplus)
            given[i] = given[i] + more
            surplus = surplus - more
    return np.array(given)


def normal_values(rng, shape, scale, most, pieces=(), kind=jnp.bfloat16):
    values = scale * jax.random.normal(rng, shape, jnp.float32)
    if pieces:
        values = values * block_scale(rng, shape, pieces, -0.22, 0.18)
    return jnp.clip(values, -most, most).astype(kind)


def setup_inputs(seed: int = 0) -> dict:
    arg_keys = jax.random.split(jax.random.key(seed), 4)
    level_set = draw_level_set(jax.random.fold_in(arg_keys[3], 71), 0)
    velocity = normal_values(arg_keys[1], (3, NX, NY, CZ), 0.15, 2.0, ((1, 32), (2, 4)))
    box_owner_keys = jax.random.split(jax.random.fold_in(arg_keys[2], 1), N_WIDE * N_NARROW * TPD // TPD)
    box_owner_turns = jax.random.permutation(jax.random.fold_in(arg_keys[2], 3), N_WIDE * N_NARROW * TPD // TPD)
    box_owner = jax.vmap(lambda own, number: shared_out(jax.random.fold_in(arg_keys[2], 2), own, number, TPD, N_WIDE, 1, CAP, 2))(box_owner_keys, box_owner_turns).reshape((N_WIDE, N_NARROW, TPD, 1))
    return {"level_set": level_set, "velocity": velocity, "box_owner": box_owner}


WENO_EPS = 1e-06
PSEUDO_STEP = 0.3

def weno_blend(parts):
    guesses = (parts[0] / 3.0 - 7.0 * parts[1] / 6.0 + 11.0 * parts[2] / 6.0, -parts[1] / 6.0 + 5.0 * parts[2] / 6.0 + parts[3] / 3.0, parts[2] / 3.0 + 5.0 * parts[3] / 6.0 - parts[4] / 6.0)
    roughness = (13.0 / 12.0 * jnp.square(parts[0] - 2.0 * parts[1] + parts[2]) + 0.25 * jnp.square(parts[0] - 4.0 * parts[1] + 3.0 * parts[2]), 13.0 / 12.0 * jnp.square(parts[1] - 2.0 * parts[2] + parts[3]) + 0.25 * jnp.square(parts[1] - parts[3]), 13.0 / 12.0 * jnp.square(parts[2] - 2.0 * parts[3] + parts[4]) + 0.25 * jnp.square(3.0 * parts[2] - 4.0 * parts[3] + parts[4]))
    weights = [ideal_share / jnp.square(WENO_EPS + rough_part) for ideal_share, rough_part in zip((0.1, 0.6, 0.3), roughness)]
    numerator = weights[0] * guesses[0] + weights[1] * guesses[1] + weights[2] * guesses[2]
    return numerator / (weights[0] + weights[1] + weights[2])

def weno_pair(padded, along):
    extent = padded.shape[along] - 6
    differences = jnp.diff(padded, axis=along)
    stencil = [lax.slice_in_dim(differences, offset, offset + extent, axis=along) for offset in range(6)]
    from_below = weno_blend(stencil[0:5])
    from_above = weno_blend([stencil[5], stencil[4], stencil[3], stencil[2], stencil[1]])
    return (from_below, from_above)

def upwind(padded, along, speed):
    from_below, from_above = weno_pair(padded, along)
    return speed * jnp.where(speed > 0, from_below, from_above)

def advect_from(field, along_x, along_y, along_z, velocity):
    speeds = velocity.astype(jnp.float32)
    change = upwind(along_x, 0, speeds[0]) + upwind(along_y, 1, speeds[1]) + upwind(along_z, 2, speeds[2])
    return field - change

def godunov_sweep(rimmed, initial):
    center = rimmed[1:-1, 1:-1, :]
    column_pad = jnp.pad(center, ((0, 0), (0, 0), (1, 1)), mode='edge')
    smooth_sign = initial / jnp.sqrt(initial * initial + 1.0)
    outside = initial > 0

    def godunov(lower_side, upper_side):
        behind = center - lower_side
        forward = upper_side - center
        outer_term = jnp.maximum(jnp.square(jnp.maximum(behind, 0.0)), jnp.square(jnp.minimum(forward, 0.0)))
        inner_term = jnp.maximum(jnp.square(jnp.minimum(behind, 0.0)), jnp.square(jnp.maximum(forward, 0.0)))
        return jnp.where(outside, outer_term, inner_term)
    squared = godunov(rimmed[:-2, 1:-1, :], rimmed[2:, 1:-1, :])
    squared = squared + godunov(rimmed[1:-1, :-2, :], rimmed[1:-1, 2:, :])
    squared = squared + godunov(column_pad[:, :, :-2], column_pad[:, :, 2:])
    return center - PSEUDO_STEP * smooth_sign * (jnp.sqrt(squared) - 1.0)

def fraction(field):
    return 0.5 - 0.5 * field / jnp.sqrt(field * field + 1.0)

def to_tiles(one_block, edge):
    sizes_a, sizes_b, sizes_c = one_block.shape
    grouped = one_block.reshape(sizes_a // edge, edge, sizes_b // edge, edge, sizes_c // edge, edge)
    return grouped.transpose(0, 2, 4, 1, 3, 5).reshape(-1, edge ** 3)

def restrict(tiles, edge):
    leading = tiles.shape[:-1]
    half_edge = edge // 2
    depth = len(leading)
    grouped = tiles.reshape(leading + (half_edge, 2, half_edge, 2, half_edge, 2))
    return lax.optimization_barrier(jnp.mean(grouped, axis=(depth + 1, depth + 3, depth + 5))).reshape(leading + (half_edge ** 3,))

def pack_matrix(one_route, owners, capacity):
    owners_list = jnp.arange(owners, dtype=jnp.int32)
    matches = (one_route[:, None] == owners_list[None, :]).astype(jnp.int32)
    earlier = jnp.cumsum(matches, axis=0) - matches
    position = lax.optimization_barrier(jnp.sum(earlier * matches, axis=1))
    target = one_route * capacity + position
    targets = jnp.arange(owners * capacity, dtype=jnp.int32)
    return (targets[:, None] == target[None, :]).astype(jnp.float32)

def reference(level_set, velocity, box_owner):
    along_x = jnp.pad(level_set, ((3, 3), (0, 0), (0, 0)), mode='wrap')
    along_y = jnp.pad(level_set, ((0, 0), (3, 3), (0, 0)), mode='wrap')
    along_z = jnp.pad(level_set, ((0, 0), (0, 0), (3, 3)), mode='edge')
    moved = advect_from(level_set, along_x, along_y, along_z, velocity)
    surface = moved
    for sweep_index in range(SWEEPS):
        rimmed = jnp.pad(surface, ((1, 1), (1, 1), (0, 0)), mode='wrap')
        surface = godunov_sweep(rimmed, moved)
    liquid = fraction(surface)
    device_blocks = liquid.reshape(N_WIDE, CX, N_NARROW, CY, CZ).transpose(0, 2, 1, 3, 4)
    device_blocks = device_blocks.reshape(N_WIDE * N_NARROW, CX, CY, CZ)
    routes_flat = box_owner.reshape(N_WIDE * N_NARROW, TPD).astype(jnp.int32)

    def per_device(pair):
        one_block, one_route = pair
        coarse = restrict(to_tiles(one_block, TILE), TILE)
        matrix = pack_matrix(one_route, N_WIDE, CAP)
        return jnp.dot(matrix, coarse, precision=lax.Precision.HIGHEST, preferred_element_type=jnp.float32)
    outgoing = lax.map(per_device, (device_blocks, routes_flat))
    outgoing = outgoing.reshape(N_WIDE, N_NARROW, N_WIDE, CAP, (TILE // 2) ** 3)
    box_fractions = outgoing.transpose(2, 1, 0, 3, 4).reshape(N_WIDE, N_NARROW, N_WIDE * CAP, (TILE // 2) ** 3)
    return (surface, box_fractions)
```

```python
import functools

import jax
import jax.numpy as jnp
from jax import lax
from jax.experimental import pallas as pl
from jax.experimental.pallas import tpu as pltpu
from jax.sharding import PartitionSpec as P

f32 = jnp.float32
EPS = 0.75e-6
CX, CY, CZ = 32, 64, 512
CAP = 20
FIELD = (38, 4, 80, 128)
HIGH = lax.Precision.HIGHEST


def lanes_iota():
    return lax.broadcasted_iota(jnp.int32, (8, 128), 1)


def lane_from(prev, cur, k, lane):
    return pltpu.roll(jnp.where(lane >= 128 - k, prev, cur), k, 1)


def lane_to(cur, nxt, k, lane):
    return pltpu.roll(jnp.where(lane < k, nxt, cur), 128 - k, 1)


def corr(E1, E2, E3, E4):
    E2s = 0.75 * E2
    E3s = 0.75 * E3
    t1 = E2 - E1
    S1 = t1 * t1 + (E2s * (t1 + E2) + EPS)
    t2 = E3 - E2
    S2 = t2 * t2 + (E2s * E3 + EPS)
    t3 = E3 - E4
    S3 = t3 * t3 + (E3s * (t3 + E3) + EPS)
    r1 = 1.0 / S1
    r2 = 1.0 / S2
    r3 = 1.0 / S3
    w1 = r1 * r1
    w2 = (6.0 * r2) * r2
    w3 = (3.0 * r3) * r3
    return (E2 + (E3 + E3)) - ((w1 + w1) * (t2 - t1) - w3 * (t2 + t3)) / (w1 + w2 + w3)


def upwind(u, dm, dp, qm2, qm1, q0, qp1, qp2):
    p = u > 0
    V3 = jnp.where(p, dm, dp)
    E1 = jnp.where(p, qm2, qp2)
    E2 = jnp.where(p, qm1, qp1)
    E4 = jnp.where(p, qp1, qm1)
    return u * V3 + (jnp.abs(u) * (1.0 / 6.0)) * corr(E1, E2, q0, E4)


def differences(fs):
    d = [fs[i + 1] - fs[i] for i in range(6)]
    q = [d[i + 1] - d[i] for i in range(5)]
    return (d[2], d[3], *q)


def advect_group(x, row, F, V, M):
    lane = lanes_iota()
    zero = jnp.zeros((8, 128), f32)
    for h in range(2):
        r = row + 8 * h + 8
        fc = [F[x + 3, c, pl.ds(r, 8), :] for c in range(4)]
        dm, dp, q = [], [], []
        for c in range(4):
            if c > 0:
                fm = lane_from(fc[c - 1], fc[c], 1, lane)
            else:
                fm = jnp.where(lane == 0, fc[0], pltpu.roll(fc[0], 1, 1))
            if c < 3:
                fp = lane_to(fc[c], fc[c + 1], 1, lane)
            else:
                fp = jnp.where(lane == 127, fc[3], pltpu.roll(fc[3], 127, 1))
            dm.append(fc[c] - fm)
            dp.append(fp - fc[c])
            q.append(dp[c] - dm[c])
        for c in range(4):
            u = V[:, x, pl.ds(row, 16), c * 128 : c * 128 + 128][:, 8 * h : 8 * h + 8].astype(f32)
            fx = [fc[c] if k == 3 else F[x + k, c, pl.ds(r, 8), :] for k in range(7)]
            acc = upwind(u[0], *differences(fx))
            fy = [fc[c] if k == 3 else F[x + 3, c, pl.ds(r + k - 3, 8), :] for k in range(7)]
            acc = acc + upwind(u[1], *differences(fy))
            qp = q[c - 1] if c > 0 else zero
            qn = q[c + 1] if c < 3 else zero
            acc = acc + upwind(
                u[2],
                dm[c],
                dp[c],
                lane_from(qp, q[c], 2, lane),
                lane_from(qp, q[c], 1, lane),
                q[c],
                lane_to(q[c], qn, 1, lane),
                lane_to(q[c], qn, 2, lane),
            )
            M[x + 3, c, pl.ds(r, 8), :] = fc[c] - acc


def pack_rows(field, buf):
    def body(k, _):
        for j in range(8):
            for c in range(4):
                for s, row in ((0, 8), (1, 69)):
                    buf[s, c, pl.ds(k * 24 + 3 * j, 3), :] = field[k * 8 + j + 3, c, row : row + 3, :]
        return 0

    lax.fori_loop(0, 4, body, 0)


def unpack_rows(field, buf):
    def body(k, _):
        for j in range(8):
            for c in range(4):
                for s, row in ((0, 5), (1, 72)):
                    field[k * 8 + j + 3, c, row : row + 3, :] = buf[s, c, pl.ds(k * 24 + 3 * j, 3), :]
        return 0

    lax.fori_loop(0, 4, body, 0)


def advect_kernel(
    nw, nn, l_ref, v_ref, m_ref, F, M, V, ys, yr, ys2, yr2, cr, lsem, vsem, osem, ssem, rsem
):
    w, n = lax.axis_index("wide"), lax.axis_index("narrow")
    left, right = lax.rem(w + nw - 1, nw), lax.rem(w + 1, nw)
    down, up = lax.rem(n + nn - 1, nn), lax.rem(n + 1, nn)

    loads = [
        pltpu.make_async_copy(
            l_ref.at[:, :, c * 128 : c * 128 + 128], F.at[3:35, c, 8:72, :], lsem.at[c]
        )
        for c in range(4)
    ]
    speeds = [
        pltpu.make_async_copy(v_ref.at[:, a:b], V.at[:, a:b], vsem.at[i])
        for i, (a, b) in enumerate(((3, 16), (0, 3), (16, 32)))
    ]
    for copy in loads + speeds:
        copy.start()

    barrier = pltpu.get_barrier_semaphore()
    around = [(a, b) for a in (left, w, right) for b in (down, n, up)]
    del around[4]
    for a, b in around:
        pl.semaphore_signal(
            barrier, inc=1, device_id={"wide": a, "narrow": b}, device_id_type=pl.DeviceIdType.MESH
        )
    pl.semaphore_wait(barrier, 8)

    def send(src, dst, k, a, b):
        return pltpu.make_async_remote_copy(
            src_ref=src,
            dst_ref=dst,
            send_sem=ssem.at[k],
            recv_sem=rsem.at[k],
            device_id={"wide": a, "narrow": b},
            device_id_type=pl.DeviceIdType.MESH,
        )

    def sides(field, sent, got, k):
        return (
            [
                send(field.at[3:6, :, 8:72, :], field.at[35:38, :, 8:72, :], k, left, n),
                send(field.at[32:35, :, 8:72, :], field.at[0:3, :, 8:72, :], k + 1, right, n),
            ],
            [
                send(sent.at[0], got.at[1], k + 2, w, down),
                send(sent.at[1], got.at[0], k + 3, w, up),
            ],
        )

    first_x, first_y = sides(F, ys, yr, 0)
    second_x, second_y = sides(M, ys2, yr2, 4)
    corners = [
        send(ys2.at[0, :, 0:16, :], cr.at[1, 1], 8, left, down),
        send(ys2.at[1, :, 0:16, :], cr.at[1, 0], 9, left, up),
        send(ys2.at[0, :, 80:96, :], cr.at[0, 1], 10, right, down),
        send(ys2.at[1, :, 80:96, :], cr.at[0, 0], 11, right, up),
    ]

    for copy in loads:
        copy.wait()
    for copy in first_x:
        copy.start()
    pack_rows(F, ys)
    for copy in first_y:
        copy.start()

    def inner(i, _):
        advect_group(3 + i // 2, pl.multiple_of(16 + 16 * (i % 2), 16), F, V, M)
        return 0

    def rims(i, _):
        advect_group(i // 2, pl.multiple_of(48 * (i % 2), 16), F, V, M)
        return 0

    def ends(i, _):
        k = i // 2
        advect_group(k + 26 * (k // 3), pl.multiple_of(16 + 16 * (i % 2), 16), F, V, M)
        return 0

    speeds[0].wait()
    lax.fori_loop(0, 26, inner, 0)
    speeds[1].wait()
    speeds[2].wait()
    for copy in first_x + first_y:
        copy.wait()
    unpack_rows(F, yr)
    lax.fori_loop(0, 64, rims, 0)
    pack_rows(M, ys2)
    for copy in second_y + corners:
        copy.start()
    lax.fori_loop(0, 12, ends, 0)
    for copy in second_x:
        copy.start()
    outs = []

    def put(k, a, b, rows):
        rows = slice(*rows)
        copy = pltpu.make_async_copy(M.at[a:b, :, rows, :], m_ref.at[a:b, :, rows, :], osem.at[k])
        copy.start()
        outs.append(copy)

    put(0, 3, 19, (8, 72))
    lax.fori_loop(26, 52, inner, 0)
    put(1, 19, 35, (8, 72))
    for copy in second_x + second_y + corners:
        copy.wait()
    unpack_rows(M, yr2)
    for xs in range(2):
        for ysd in range(2):
            for j in range(3):
                row = (5, 72)[ysd]
                at = (7, 0)[xs] + 3 * j
                for c in range(4):
                    M[35 * xs + j, c, row : row + 3, :] = cr[xs, ysd, c, at : at + 3, :]
    put(2, 0, 3, (8, 72))
    put(3, 35, 38, (8, 72))
    put(4, 0, 38, (0, 8))
    put(5, 0, 38, (72, 80))
    for copy in outs:
        copy.wait()


def advect(level_set, velocity, nw, nn):
    return pl.pallas_call(
        functools.partial(advect_kernel, nw, nn),
        out_shape=jax.ShapeDtypeStruct(FIELD, f32),
        in_specs=[pl.BlockSpec(memory_space=pl.ANY)] * 2,
        out_specs=pl.BlockSpec(memory_space=pl.ANY),
        scratch_shapes=[
            pltpu.VMEM(FIELD, f32),
            pltpu.VMEM(FIELD, f32),
            pltpu.VMEM((3, CX, CY, CZ), jnp.bfloat16),
            pltpu.VMEM((2, 4, 96, 128), f32),
            pltpu.VMEM((2, 4, 96, 128), f32),
            pltpu.VMEM((2, 4, 96, 128), f32),
            pltpu.VMEM((2, 4, 96, 128), f32),
            pltpu.VMEM((2, 2, 4, 16, 128), f32),
            pltpu.SemaphoreType.DMA((4,)),
            pltpu.SemaphoreType.DMA((3,)),
            pltpu.SemaphoreType.DMA((6,)),
            pltpu.SemaphoreType.DMA((12,)),
            pltpu.SemaphoreType.DMA((12,)),
        ],
        compiler_params=pltpu.CompilerParams(
            collective_id=0, has_side_effects=True, vmem_limit_bytes=48 << 20
        ),
        name="advect",
    )(level_set, velocity)


def sweep_block(x, r, src, dst, S, lane, moved=None):
    fc = [src[x, c, pl.ds(r, 8), :] for c in range(4)]
    new = []
    for c in range(4):
        cur = fc[c]
        if moved is None:
            s = S[x, c, pl.ds(r, 8), :]
        else:
            s = (0.3 * cur) * lax.rsqrt(cur * cur + 1.0)
            S[x, c, pl.ds(r, 8), :] = s
        sg = jnp.where(s > 0, 1.0, -1.0)
        sc = sg * cur

        def term(lo, hi):
            e = sc - jnp.minimum(jnp.minimum(sg * lo, sg * hi), sc)
            return e * e

        G = term(src[x - 1, c, pl.ds(r, 8), :], src[x + 1, c, pl.ds(r, 8), :])
        G = G + term(src[x, c, pl.ds(r - 1, 8), :], src[x, c, pl.ds(r + 1, 8), :])
        if c > 0:
            lo = lane_from(fc[c - 1], cur, 1, lane)
        else:
            lo = jnp.where(lane == 0, cur, pltpu.roll(cur, 1, 1))
        if c < 3:
            hi = lane_to(cur, fc[c + 1], 1, lane)
        else:
            hi = jnp.where(lane == 127, cur, pltpu.roll(cur, 127, 1))
        G = G + term(lo, hi)
        root = G * lax.rsqrt(jnp.maximum(G, 1e-37))
        new.append(cur - s * (root - 1.0))
    return new


def sweep_kernel(nw, m_ref, route_ref, surf_ref, out_ref, M, A, B, S, O, H, Q, C, msem, osem):
    loads = [
        pltpu.make_async_copy(m_ref.at[a : a + 19], M.at[a : a + 19], msem.at[a // 19])
        for a in (0, 19)
    ]
    for copy in loads:
        copy.start()
    lane = lanes_iota()

    def sweep(src, dst, row0, first):
        def body(x, _):
            for b in range(9):
                r = row0 + 8 * b
                new = sweep_block(x, r, src, dst, S, lane, True if first else None)
                for c in range(4):
                    dst[x, c, pl.ds(r, 8), :] = new[c]
            return 0

        return body

    loads[0].wait()
    lax.fori_loop(1, 18, sweep(M, A, 6, True), 0)
    loads[1].wait()
    lax.fori_loop(18, 37, sweep(M, A, 6, True), 0)
    lax.fori_loop(2, 36, sweep(A, B, 7, False), 0)

    def last(i, _):
        for b in range(8):
            r = 8 + 8 * b
            both = []
            for half in range(2):
                x = 3 + 2 * i + half
                new = sweep_block(x, r, B, None, S, lane)
                for c in range(4):
                    O[2 * i + half, c, pl.ds(r - 8, 8), :] = new[c]
                both.append([v * lax.rsqrt(v * v + 1.0) for v in new])
            for c in range(4):
                H[c, pl.ds(r - 8, 8), :] = both[0][c] + both[1][c]
        for yt in range(4):
            row = pl.multiple_of((i // 8) * 256 + yt * 64 + (i % 8) * 8, 8)
            for c in range(4):
                Q[pl.ds(row, 8), c * 128 : c * 128 + 128] = (
                    H[c, pl.ds(16 * yt, 8, stride=2), :] + H[c, pl.ds(16 * yt + 1, 8, stride=2), :]
                )
        for c in range(4):
            pltpu.make_async_copy(
                O.at[pl.ds(2 * i, 2), c],
                surf_ref.at[pl.ds(2 * i, 2), :, c * 128 : c * 128 + 128],
                osem.at[c],
            ).start()
        return 0

    lax.fori_loop(0, 16, last, 0)

    def iota(shape, dim):
        return lax.broadcasted_iota(jnp.int32, shape, dim)

    fine = iota((512, 128), 0) // 2
    col = iota((512, 128), 1)
    base = (col % 32) * 8 + (col // 32) * 2
    pools = [(fine == base + e).astype(f32) for e in range(2)]
    for b in range(8):
        block = Q[64 * b : 64 * b + 64, :]
        halves = [
            jnp.dot(block, pool, precision=HIGH, preferred_element_type=f32) for pool in pools
        ]
        turned = jnp.concatenate(halves, axis=0).T
        for h in range(4):
            C[32 * b : 32 * b + 32, 128 * h : 128 * h + 128] = turned[32 * h : 32 * h + 32, :]
    j = iota((512, 512), 1)
    order = (iota((512, 512), 0) == (j % 8) * 64 + j // 8).astype(f32)
    coarse = 0.5 - 0.0625 * jnp.dot(C[...], order, precision=HIGH, preferred_element_type=f32)
    tiles = route_ref.shape[1]
    route = route_ref[...]
    matches = (route == iota((nw, tiles), 0)).astype(f32)
    before = (iota((tiles, tiles), 0) < iota((tiles, tiles), 1)).astype(f32)
    earlier = jnp.dot(matches, before, precision=HIGH, preferred_element_type=f32)
    position = jnp.sum(earlier * matches, axis=0, keepdims=True).astype(jnp.int32)
    target = route * 24 + position
    matrix = (iota((nw * 24, tiles), 0) == target).astype(f32)
    packed = jnp.dot(matrix, coarse, precision=HIGH, preferred_element_type=f32)
    for d in range(nw):
        out_ref[d] = packed[24 * d : 24 * d + CAP, :]
    for c in range(4):
        pltpu.make_async_copy(O.at[:, c], surf_ref.at[:, :, c * 128 : c * 128 + 128], osem.at[c]).wait()


def sweeps(moved, route, nw):
    return pl.pallas_call(
        functools.partial(sweep_kernel, nw),
        out_shape=(
            jax.ShapeDtypeStruct((CX, CY, CZ), f32),
            jax.ShapeDtypeStruct((nw, CAP, 512), f32),
        ),
        in_specs=[pl.BlockSpec(memory_space=pl.ANY), pl.BlockSpec(memory_space=pltpu.VMEM)],
        out_specs=(pl.BlockSpec(memory_space=pl.ANY), pl.BlockSpec(memory_space=pltpu.VMEM)),
        scratch_shapes=[
            pltpu.VMEM(FIELD, f32),
            pltpu.VMEM(FIELD, f32),
            pltpu.VMEM(FIELD, f32),
            pltpu.VMEM(FIELD, f32),
            pltpu.VMEM((CX, 4, CY, 128), f32),
            pltpu.VMEM((4, CY, 128), f32),
            pltpu.VMEM((512, 512), f32),
            pltpu.VMEM((256, 512), f32),
            pltpu.SemaphoreType.DMA((2,)),
            pltpu.SemaphoreType.DMA((4,)),
        ],
        compiler_params=pltpu.CompilerParams(vmem_limit_bytes=60 << 20),
        name="sweeps",
    )(moved, route)


def exchange_kernel(nw, src, dst, own_sem, ssem, rsem):
    w = lax.axis_index("wide")
    own = pltpu.make_async_copy(src.at[w], dst.at[w], own_sem)
    own.start()
    barrier = pltpu.get_barrier_semaphore()

    def greet(i, _):
        pl.semaphore_signal(
            barrier,
            inc=1,
            device_id={"wide": lax.rem(w + i, nw)},
            device_id_type=pl.DeviceIdType.MESH,
        )
        return 0

    lax.fori_loop(1, nw, greet, 0)
    pl.semaphore_wait(barrier, nw - 1)

    def copy(i):
        to = lax.rem(w + i, nw)
        return pltpu.make_async_remote_copy(
            src_ref=src.at[to],
            dst_ref=dst.at[w],
            send_sem=ssem.at[i],
            recv_sem=rsem.at[i],
            device_id={"wide": to},
            device_id_type=pl.DeviceIdType.MESH,
        )

    def send(i, _):
        copy(i).start()
        return 0

    lax.fori_loop(1, nw, send, 0)

    def finish(i, _):
        copy(i).wait()
        return 0

    lax.fori_loop(1, nw, finish, 0)
    own.wait()


def exchange(outgoing, nw):
    return pl.pallas_call(
        functools.partial(exchange_kernel, nw),
        out_shape=jax.ShapeDtypeStruct(outgoing.shape, f32),
        in_specs=[pl.BlockSpec(memory_space=pl.ANY)],
        out_specs=pl.BlockSpec(memory_space=pl.ANY),
        scratch_shapes=[
            pltpu.SemaphoreType.DMA,
            pltpu.SemaphoreType.DMA((nw,)),
            pltpu.SemaphoreType.DMA((nw,)),
        ],
        compiler_params=pltpu.CompilerParams(collective_id=1, has_side_effects=True),
        name="exchange",
    )(outgoing)


def solution(mesh):
    nw, nn = mesh.shape["wide"], mesh.shape["narrow"]

    def on_device(level_set, velocity, box_owner):
        moved = advect(level_set, velocity, nw, nn)
        surface, outgoing = sweeps(moved, box_owner.reshape(1, -1), nw)
        slots = exchange(outgoing, nw)
        return surface, slots.reshape(1, 1, nw * CAP, 512)

    return jax.shard_map(
        on_device,
        mesh=mesh,
        in_specs=(
            P("wide", "narrow", None),
            P(None, "wide", "narrow", None),
            P("wide", "narrow", None, None),
        ),
        out_specs=(P("wide", "narrow", None), P("wide", "narrow", None, None)),
        check_vma=False,
    )
```

```python
import functools

import jax
import jax.numpy as jnp
from jax import lax
from jax.experimental import pallas as pl
from jax.experimental.pallas import tpu as pltpu
from jax.sharding import PartitionSpec as P

f32 = jnp.float32
EPS = 0.75e-6
CX, CY, CZ = 32, 64, 512
CAP = 20
FIELD = (38, 4, 80, 128)


def lanes_iota():
    return lax.broadcasted_iota(jnp.int32, (8, 128), 1)


def lane_from(prev, cur, k, lane):
    return pltpu.roll(jnp.where(lane >= 128 - k, prev, cur), k, 1)


def lane_to(cur, nxt, k, lane):
    return pltpu.roll(jnp.where(lane < k, nxt, cur), 128 - k, 1)


def corr(E1, E2, E3, E4):
    E2s = 0.75 * E2
    E3s = 0.75 * E3
    t1 = E2 - E1
    S1 = t1 * t1 + (E2s * (t1 + E2) + EPS)
    t2 = E3 - E2
    S2 = t2 * t2 + (E2s * E3 + EPS)
    t3 = E3 - E4
    S3 = t3 * t3 + (E3s * (t3 + E3) + EPS)
    r1 = 1.0 / S1
    r2 = 1.0 / S2
    r3 = 1.0 / S3
    w1 = r1 * r1
    w2 = (6.0 * r2) * r2
    w3 = (3.0 * r3) * r3
    return (E2 + (E3 + E3)) - ((w1 + w1) * (t2 - t1) - w3 * (t2 + t3)) / (w1 + w2 + w3)


def upwind(u, dm, dp, qm2, qm1, q0, qp1, qp2):
    p = u > 0
    V3 = jnp.where(p, dm, dp)
    E1 = jnp.where(p, qm2, qp2)
    E2 = jnp.where(p, qm1, qp1)
    E4 = jnp.where(p, qp1, qm1)
    return u * V3 + (jnp.abs(u) * (1.0 / 6.0)) * corr(E1, E2, q0, E4)


def differences(fs):
    d = [fs[i + 1] - fs[i] for i in range(6)]
    q = [d[i + 1] - d[i] for i in range(5)]
    return (d[2], d[3], *q)


def advect_group(x, row, F, V, M):
    lane = lanes_iota()
    zero = jnp.zeros((8, 128), f32)
    for h in range(2):
        r = row + 8 * h + 8
        fc = [F[x + 3, c, pl.ds(r, 8), :] for c in range(4)]
        dm, dp, q = [], [], []
        for c in range(4):
            if c > 0:
                fm = lane_from(fc[c - 1], fc[c], 1, lane)
            else:
                fm = jnp.where(lane == 0, fc[0], pltpu.roll(fc[0], 1, 1))
            if c < 3:
                fp = lane_to(fc[c], fc[c + 1], 1, lane)
            else:
                fp = jnp.where(lane == 127, fc[3], pltpu.roll(fc[3], 127, 1))
            dm.append(fc[c] - fm)
            dp.append(fp - fc[c])
            q.append(dp[c] - dm[c])
        for c in range(4):
            u = V[:, x, pl.ds(row, 16), c * 128 : c * 128 + 128][:, 8 * h : 8 * h + 8].astype(f32)
            fx = [fc[c] if k == 3 else F[x + k, c, pl.ds(r, 8), :] for k in range(7)]
            acc = upwind(u[0], *differences(fx))
            fy = [fc[c] if k == 3 else F[x + 3, c, pl.ds(r + k - 3, 8), :] for k in range(7)]
            acc = acc + upwind(u[1], *differences(fy))
            qp = q[c - 1] if c > 0 else zero
            qn = q[c + 1] if c < 3 else zero
            acc = acc + upwind(
                u[2],
                dm[c],
                dp[c],
                lane_from(qp, q[c], 2, lane),
                lane_from(qp, q[c], 1, lane),
                q[c],
                lane_to(q[c], qn, 1, lane),
                lane_to(q[c], qn, 2, lane),
            )
            M[x + 3, c, pl.ds(r, 8), :] = fc[c] - acc


def pack_rows(field, buf):
    def body(k, _):
        for j in range(8):
            for c in range(4):
                for s, row in ((0, 8), (1, 69)):
                    buf[s, c, pl.ds(k * 24 + 3 * j, 3), :] = field[k * 8 + j + 3, c, row : row + 3, :]
        return 0

    lax.fori_loop(0, 4, body, 0)


def unpack_rows(field, buf):
    def body(k, _):
        for j in range(8):
            for c in range(4):
                for s, row in ((0, 5), (1, 72)):
                    field[k * 8 + j + 3, c, row : row + 3, :] = buf[s, c, pl.ds(k * 24 + 3 * j, 3), :]
        return 0

    lax.fori_loop(0, 4, body, 0)


def sweep_block(x, r, src, dst, S, lane, moved=None):
    fc = [src[x, c, pl.ds(r, 8), :] for c in range(4)]
    new = []
    for c in range(4):
        cur = fc[c]
        if moved is None:
            s = S[x, c, pl.ds(r, 8), :]
        else:
            s = (0.3 * cur) * lax.rsqrt(cur * cur + 1.0)
            S[x, c, pl.ds(r, 8), :] = s
        sg = jnp.where(s > 0, 1.0, -1.0)
        sc = sg * cur

        def term(lo, hi):
            e = sc - jnp.minimum(jnp.minimum(sg * lo, sg * hi), sc)
            return e * e

        G = term(src[x - 1, c, pl.ds(r, 8), :], src[x + 1, c, pl.ds(r, 8), :])
        G = G + term(src[x, c, pl.ds(r - 1, 8), :], src[x, c, pl.ds(r + 1, 8), :])
        if c > 0:
            lo = lane_from(fc[c - 1], cur, 1, lane)
        else:
            lo = jnp.where(lane == 0, cur, pltpu.roll(cur, 1, 1))
        if c < 3:
            hi = lane_to(cur, fc[c + 1], 1, lane)
        else:
            hi = jnp.where(lane == 127, cur, pltpu.roll(cur, 127, 1))
        G = G + term(lo, hi)
        root = G * lax.rsqrt(jnp.maximum(G, 1e-37))
        new.append(cur - s * (root - 1.0))
    return new


def iota(shape, dim):
    return lax.broadcasted_iota(jnp.int32, shape, dim)


def place_tiles(route_ref, X, nw):
    tiles = route_ref.shape[1]
    route = route_ref[...]
    matches = (route == iota((nw, tiles), 0)).astype(f32)
    before = (iota((tiles, tiles), 0) < iota((tiles, tiles), 1)).astype(f32)
    earlier = jnp.dot(
        matches.astype(jnp.bfloat16), before.astype(jnp.bfloat16), preferred_element_type=f32
    )
    position = jnp.sum(earlier * matches, axis=0, keepdims=True).astype(jnp.int32)
    target = route * 24 + position
    X[...] = (iota((nw * 24, tiles), 0) == target).astype(f32).astype(jnp.bfloat16)


def gather_tiles(Q, T, C):
    for c in range(4):
        T[c * 128 : c * 128 + 128, :] = Q[c].T
    lane = lanes_iota()
    for zv in range(4):
        part = [
            T[pl.ds(128 * zv + 2 * z, 8, stride=16), :] + T[pl.ds(128 * zv + 2 * z + 1, 8, stride=16), :]
            for z in range(8)
        ]
        for s in (1, 2, 4):
            bit = (lane & s) > 0
            for z in range(8):
                if z & s == 0:
                    a, b = part[z], part[z | s]
                    part[z] = jnp.where(bit, pltpu.roll(b, s, 1), a)
                    part[z | s] = jnp.where(bit, b, pltpu.roll(a, 128 - s, 1))
        for t in range(8):
            C[32 * t + 8 * zv : 32 * t + 8 * zv + 8, :] = 0.5 - 0.0625 * part[t]


def pack_tiles(X, C, G, nw):
    rest = C[...]
    packed = None
    for _ in range(3):
        term = rest.astype(jnp.bfloat16)
        rest = rest - term.astype(f32)
        product = jnp.dot(X[...], term, preferred_element_type=f32)
        packed = product if packed is None else packed + product
    for d in range(nw):
        G[d] = packed[24 * d : 24 * d + CAP, :]


def kernel(
    nw, nn, l_ref, v_ref, route_ref, surf_ref, out_ref,
    F, M, V, S, O, ys, yr, ys2, yr2, cr, H, Q, T, C, X, G,
    lsem, vsem, osem, own_sem, ssem, rsem, tsem, usem,
):
    w, n = lax.axis_index("wide"), lax.axis_index("narrow")
    left, right = lax.rem(w + nw - 1, nw), lax.rem(w + 1, nw)
    down, up = lax.rem(n + nn - 1, nn), lax.rem(n + 1, nn)
    lane = lanes_iota()

    loads = [
        pltpu.make_async_copy(
            l_ref.at[:, :, c * 128 : c * 128 + 128], F.at[3:35, c, 8:72, :], lsem.at[c]
        )
        for c in range(4)
    ]
    speeds = [
        pltpu.make_async_copy(v_ref.at[:, a:b], V.at[:, a:b], vsem.at[i])
        for i, (a, b) in enumerate(((3, 16), (0, 3), (16, 32)))
    ]
    for copy in loads + speeds:
        copy.start()

    barrier = pltpu.get_barrier_semaphore()

    def greet(a, b):
        pl.semaphore_signal(
            barrier, inc=1, device_id={"wide": a, "narrow": b}, device_id_type=pl.DeviceIdType.MESH
        )

    def greet_wide(i, _):
        greet(lax.rem(w + i, nw), n)
        return 0

    lax.fori_loop(1, nw, greet_wide, 0)
    for a in (left, w, right):
        for b in (down, up):
            greet(a, b)
    pl.semaphore_wait(barrier, nw - 1 + 6)

    def send(src, dst, k, a, b):
        return pltpu.make_async_remote_copy(
            src_ref=src,
            dst_ref=dst,
            send_sem=ssem.at[k],
            recv_sem=rsem.at[k],
            device_id={"wide": a, "narrow": b},
            device_id_type=pl.DeviceIdType.MESH,
        )

    def sides(field, sent, got, k):
        return (
            [
                send(field.at[3:6, :, 8:72, :], field.at[35:38, :, 8:72, :], k, left, n),
                send(field.at[32:35, :, 8:72, :], field.at[0:3, :, 8:72, :], k + 1, right, n),
            ],
            [
                send(sent.at[0], got.at[1], k + 2, w, down),
                send(sent.at[1], got.at[0], k + 3, w, up),
            ],
        )

    first_x, first_y = sides(F, ys, yr, 0)
    second_x, second_y = sides(M, ys2, yr2, 4)
    corners = [
        send(ys2.at[0, :, 0:16, :], cr.at[1, 1], 8, left, down),
        send(ys2.at[1, :, 0:16, :], cr.at[1, 0], 9, left, up),
        send(ys2.at[0, :, 80:96, :], cr.at[0, 1], 10, right, down),
        send(ys2.at[1, :, 80:96, :], cr.at[0, 0], 11, right, up),
    ]

    for copy in loads:
        copy.wait()
    for copy in first_x:
        copy.start()
    pack_rows(F, ys)
    for copy in first_y:
        copy.start()
    place_tiles(route_ref, X, nw)

    def inner(i, _):
        advect_group(3 + i // 2, pl.multiple_of(16 + 16 * (i % 2), 16), F, V, M)
        return 0

    def rims(i, _):
        advect_group(i // 2, pl.multiple_of(48 * (i % 2), 16), F, V, M)
        return 0

    def ends(i, _):
        k = i // 2
        advect_group(k + 26 * (k // 3), pl.multiple_of(16 + 16 * (i % 2), 16), F, V, M)
        return 0

    speeds[0].wait()
    lax.fori_loop(0, 26, inner, 0)
    speeds[1].wait()
    speeds[2].wait()
    for copy in first_x + first_y:
        copy.wait()
    unpack_rows(F, yr)
    lax.fori_loop(0, 64, rims, 0)
    pack_rows(M, ys2)
    for copy in second_y + corners:
        copy.start()
    lax.fori_loop(0, 12, ends, 0)
    for copy in second_x:
        copy.start()
    lax.fori_loop(26, 52, inner, 0)
    for copy in second_x + second_y + corners:
        copy.wait()
    unpack_rows(M, yr2)
    for xs in range(2):
        for ysd in range(2):
            for j in range(3):
                row = (5, 72)[ysd]
                at = (7, 0)[xs] + 3 * j
                for c in range(4):
                    M[35 * xs + j, c, row : row + 3, :] = cr[xs, ysd, c, at : at + 3, :]

    def sweep(src, dst, row0, first, count, planes):
        def body(i, _):
            x = planes(i)
            for b in range(9):
                r = row0 + 8 * b
                new = sweep_block(x, r, src, dst, S, lane, True if first else None)
                for c in range(4):
                    dst[x, c, pl.ds(r, 8), :] = new[c]
            return 0

        lax.fori_loop(0, count, body, 0)

    def two(start, count):
        return 2 * count, lambda i: start + lax.rem(i, count) + 16 * (i // count)

    def last_sweep(q):
        def body(i, _):
            tile, pair = i // 2, lax.rem(i, 2)
            x0 = 4 * q + 2 * pair + 16 * tile
            for b in range(8):
                both = []
                for half in range(2):
                    new = sweep_block(x0 + half + 3, 8 + 8 * b, M, None, S, lane)
                    for c in range(4):
                        O[x0 + half, c, 8 * b : 8 * b + 8, :] = new[c]
                    both.append([v * lax.rsqrt(v * v + 1.0) for v in new])
                for c in range(4):
                    H[c, 8 * b : 8 * b + 8, :] = both[0][c] + both[1][c]
            for yt in range(4):
                for c in range(4):
                    Q[c, pl.ds(pair * 64 + tile * 4 + yt, 8, stride=8), :] = (
                        H[c, pl.ds(16 * yt, 8, stride=2), :]
                        + H[c, pl.ds(16 * yt + 1, 8, stride=2), :]
                    )
            for c in range(4):
                pltpu.make_async_copy(
                    O.at[pl.ds(x0, 2), c],
                    surf_ref.at[pl.ds(x0, 2), :, c * 128 : c * 128 + 128],
                    osem.at[c],
                ).start()
            return 0

        lax.fori_loop(0, 4, body, 0)

    def tile_copy(q, i):
        to = lax.rem(w + i, nw)
        return pltpu.make_async_remote_copy(
            src_ref=G.at[q, to],
            dst_ref=out_ref.at[w, :, q * 128 : q * 128 + 128],
            send_sem=tsem.at[q, i],
            recv_sem=usem.at[q, i],
            device_id={"wide": to},
            device_id_type=pl.DeviceIdType.MESH,
        )

    own = []
    for q in range(4):
        if q == 0:
            sweep(M, F, 6, True, *two(1, 8))
            sweep(F, M, 7, False, *two(2, 6))
        elif q < 3:
            sweep(M, F, 6, True, *two(4 * q + 5, 4))
            sweep(F, M, 7, False, *two(4 * q + 4, 4))
        else:
            sweep(M, F, 6, True, 4, lambda i: i + 33)
            sweep(F, M, 7, False, 6, lambda i: i + 16 + 14 * ((i + 2) // 4))
        last_sweep(q)
        gather_tiles(Q, T, C)
        pack_tiles(X, C, G.at[q], nw)

        def start(i, _):
            tile_copy(q, i).start()
            return 0

        lax.fori_loop(1, nw, start, 0)
        own.append(
            pltpu.make_async_copy(
                G.at[q, w], out_ref.at[w, :, q * 128 : q * 128 + 128], own_sem.at[q]
            )
        )
        own[-1].start()

    for q in range(4):

        def finish(i, _):
            tile_copy(q, i).wait()
            return 0

        lax.fori_loop(1, nw, finish, 0)
        own[q].wait()
    for c in range(4):
        pltpu.make_async_copy(O.at[:, c], surf_ref.at[:, :, c * 128 : c * 128 + 128], osem.at[c]).wait()


def solution(mesh):
    nw, nn = mesh.shape["wide"], mesh.shape["narrow"]
    rows = pltpu.VMEM((2, 4, 96, 128), f32)
    dma = pltpu.SemaphoreType.DMA
    hbm = pl.BlockSpec(memory_space=pl.ANY)
    call = pl.pallas_call(
        functools.partial(kernel, nw, nn),
        out_shape=(
            jax.ShapeDtypeStruct((CX, CY, CZ), f32),
            jax.ShapeDtypeStruct((nw, CAP, 512), f32),
        ),
        in_specs=[hbm, hbm, pl.BlockSpec(memory_space=pltpu.VMEM)],
        out_specs=(hbm, hbm),
        scratch_shapes=[
            pltpu.VMEM(FIELD, f32),
            pltpu.VMEM(FIELD, f32),
            pltpu.VMEM((3, CX, CY, CZ), jnp.bfloat16),
            pltpu.VMEM(FIELD, f32),
            pltpu.VMEM((CX, 4, CY, 128), f32),
            rows,
            rows,
            rows,
            rows,
            pltpu.VMEM((2, 2, 4, 16, 128), f32),
            pltpu.VMEM((4, CY, 128), f32),
            pltpu.VMEM((4, 128, 128), f32),
            pltpu.VMEM((512, 128), f32),
            pltpu.VMEM((256, 128), f32),
            pltpu.VMEM((nw * 24, 256), jnp.bfloat16),
            pltpu.VMEM((4, nw, CAP, 128), f32),
            dma((4,)),
            dma((3,)),
            dma((4,)),
            dma((4,)),
            dma((12,)),
            dma((12,)),
            dma((4, nw)),
            dma((4, nw)),
        ],
        compiler_params=pltpu.CompilerParams(
            collective_id=0, has_side_effects=True, vmem_limit_bytes=60 << 20
        ),
        name="level_set_step",
    )

    def on_device(level_set, velocity, box_owner):
        surface, slots = call(level_set, velocity, box_owner.reshape(1, -1))
        return surface, slots.reshape(1, 1, nw * CAP, 512)

    return jax.shard_map(
        on_device,
        mesh=mesh,
        in_specs=(
            P("wide", "narrow", None),
            P(None, "wide", "narrow", None),
            P("wide", "narrow", None, None),
        ),
        out_specs=(P("wide", "narrow", None), P("wide", "narrow", None, None)),
        check_vma=False,
    )
```

```python
import functools

import jax
import jax.numpy as jnp
from jax import lax
from jax.experimental import pallas as pl
from jax.experimental.pallas import tpu as pltpu
from jax.sharding import PartitionSpec as P

f32 = jnp.float32
EPS = 0.75e-6
CX, CY, CZ = 32, 64, 512
CAP = 20
FIELD = (38, 4, 80, 128)


def lanes_iota():
    return lax.broadcasted_iota(jnp.int32, (8, 128), 1)


def lane_from(prev, cur, k, lane):
    return pltpu.roll(jnp.where(lane >= 128 - k, prev, cur), k, 1)


def lane_to(cur, nxt, k, lane):
    return pltpu.roll(jnp.where(lane < k, nxt, cur), 128 - k, 1)


def corr(E1, E2, E3, E4):
    E2s = 0.75 * E2
    E3s = 0.75 * E3
    t1 = E2 - E1
    S1 = t1 * t1 + (E2s * (t1 + E2) + EPS)
    t2 = E3 - E2
    S2 = t2 * t2 + (E2s * E3 + EPS)
    t3 = E3 - E4
    S3 = t3 * t3 + (E3s * (t3 + E3) + EPS)
    r1 = 1.0 / S1
    r2 = 1.0 / S2
    r3 = 1.0 / S3
    w1 = r1 * r1
    w2 = (6.0 * r2) * r2
    w3 = (3.0 * r3) * r3
    return (E2 + (E3 + E3)) - ((w1 + w1) * (t2 - t1) - w3 * (t2 + t3)) / (w1 + w2 + w3)


def upwind(u, dm, dp, qm2, qm1, q0, qp1, qp2):
    p = u > 0
    V3 = jnp.where(p, dm, dp)
    E1 = jnp.where(p, qm2, qp2)
    E2 = jnp.where(p, qm1, qp1)
    E4 = jnp.where(p, qp1, qm1)
    return u * V3 + (jnp.abs(u) * (1.0 / 6.0)) * corr(E1, E2, q0, E4)


def differences(fs):
    d = [fs[i + 1] - fs[i] for i in range(6)]
    q = [d[i + 1] - d[i] for i in range(5)]
    return (d[2], d[3], *q)


def third_differences(x, row, F, Z):
    lane = lanes_iota()
    for h in range(2):
        fc = [F[x + 3, c, pl.ds(row + 8 * h + 8, 8), :] for c in range(4)]
        for c in range(4):
            if c > 0:
                fm = lane_from(fc[c - 1], fc[c], 1, lane)
            else:
                fm = jnp.where(lane == 0, fc[0], pltpu.roll(fc[0], 1, 1))
            if c < 3:
                fp = lane_to(fc[c], fc[c + 1], 1, lane)
            else:
                fp = jnp.where(lane == 127, fc[3], pltpu.roll(fc[3], 127, 1))
            dm = fc[c] - fm
            Z[0, c, 8 * h : 8 * h + 8, :] = (fp - fc[c]) - dm
            Z[1, c, 8 * h : 8 * h + 8, :] = dm


def advect_group(x, row, F, V, M, Z):
    lane = lanes_iota()
    zero = jnp.zeros((8, 128), f32)
    for h in range(2):
        r = row + 8 * h + 8
        q = [zero, *(Z[0, c, 8 * h : 8 * h + 8, :] for c in range(4)), zero]
        for c in range(4):
            f = F[x + 3, c, pl.ds(r, 8), :]
            u = V[:, x, pl.ds(row, 16), c * 128 : c * 128 + 128][:, 8 * h : 8 * h + 8].astype(f32)
            fx = [f if k == 3 else F[x + k, c, pl.ds(r, 8), :] for k in range(7)]
            acc = upwind(u[0], *differences(fx))
            fy = [f if k == 3 else F[x + 3, c, pl.ds(r + k - 3, 8), :] for k in range(7)]
            acc = acc + upwind(u[1], *differences(fy))
            dm = Z[1, c, 8 * h : 8 * h + 8, :]
            qp, qc, qn = q[c : c + 3]
            acc = acc + upwind(
                u[2],
                dm,
                dm + qc,
                lane_from(qp, qc, 2, lane),
                lane_from(qp, qc, 1, lane),
                qc,
                lane_to(qc, qn, 1, lane),
                lane_to(qc, qn, 2, lane),
            )
            M[x + 3, c, pl.ds(r, 8), :] = f - acc


def advect_groups(count, place, F, V, M, Z):
    third_differences(*place(0), F, Z.at[0])

    def body(i, _):
        advect_group(*place(i), F, V, M, Z.at[lax.rem(i, 2)])
        third_differences(*place(lax.rem(i + 1, count)), F, Z.at[lax.rem(i + 1, 2)])
        return 0

    lax.fori_loop(0, count, body, 0)


def pack_rows(field, buf):
    def body(k, _):
        for j in range(8):
            for c in range(4):
                for s, row in ((0, 8), (1, 69)):
                    buf[s, c, pl.ds(k * 24 + 3 * j, 3), :] = field[k * 8 + j + 3, c, row : row + 3, :]
        return 0

    lax.fori_loop(0, 4, body, 0)


def unpack_rows(field, buf):
    def body(k, _):
        for j in range(8):
            for c in range(4):
                for s, row in ((0, 5), (1, 72)):
                    field[k * 8 + j + 3, c, row : row + 3, :] = buf[s, c, pl.ds(k * 24 + 3 * j, 3), :]
        return 0

    lax.fori_loop(0, 4, body, 0)


def sweep_block(x, r, src, dst, S, lane, moved=None):
    fc = [src[x, c, pl.ds(r, 8), :] for c in range(4)]
    new = []
    for c in range(4):
        cur = fc[c]
        if moved is None:
            s = S[x, c, pl.ds(r, 8), :]
        else:
            s = (0.3 * cur) * lax.rsqrt(cur * cur + 1.0)
            S[x, c, pl.ds(r, 8), :] = s
        sg = jnp.where(s > 0, 1.0, -1.0)
        sc = sg * cur

        def term(lo, hi):
            e = sc - jnp.minimum(jnp.minimum(sg * lo, sg * hi), sc)
            return e * e

        G = term(src[x - 1, c, pl.ds(r, 8), :], src[x + 1, c, pl.ds(r, 8), :])
        G = G + term(src[x, c, pl.ds(r - 1, 8), :], src[x, c, pl.ds(r + 1, 8), :])
        if c > 0:
            lo = lane_from(fc[c - 1], cur, 1, lane)
        else:
            lo = jnp.where(lane == 0, cur, pltpu.roll(cur, 1, 1))
        if c < 3:
            hi = lane_to(cur, fc[c + 1], 1, lane)
        else:
            hi = jnp.where(lane == 127, cur, pltpu.roll(cur, 127, 1))
        G = G + term(lo, hi)
        root = G * lax.rsqrt(jnp.maximum(G, 1e-37))
        new.append(cur - s * (root - 1.0))
    return new


def iota(shape, dim):
    return lax.broadcasted_iota(jnp.int32, shape, dim)


def place_tiles(route_ref, X, nw):
    tiles = route_ref.shape[1]
    route = route_ref[...]
    matches = (route == iota((nw, tiles), 0)).astype(f32)
    before = (iota((tiles, tiles), 0) < iota((tiles, tiles), 1)).astype(f32)
    earlier = jnp.dot(
        matches.astype(jnp.bfloat16), before.astype(jnp.bfloat16), preferred_element_type=f32
    )
    position = jnp.sum(earlier * matches, axis=0, keepdims=True).astype(jnp.int32)
    target = route * 24 + position
    X[...] = (iota((nw * 24, tiles), 0) == target).astype(f32).astype(jnp.bfloat16)


def gather_tiles(Q, T, C):
    for c in range(4):
        T[c * 128 : c * 128 + 128, :] = Q[c].T
    lane = lanes_iota()
    for zv in range(4):
        part = [
            T[pl.ds(128 * zv + 2 * z, 8, stride=16), :] + T[pl.ds(128 * zv + 2 * z + 1, 8, stride=16), :]
            for z in range(8)
        ]
        for s in (1, 2, 4):
            bit = (lane & s) > 0
            for z in range(8):
                if z & s == 0:
                    a, b = part[z], part[z | s]
                    part[z] = jnp.where(bit, pltpu.roll(b, s, 1), a)
                    part[z | s] = jnp.where(bit, b, pltpu.roll(a, 128 - s, 1))
        for t in range(8):
            C[32 * t + 8 * zv : 32 * t + 8 * zv + 8, :] = 0.5 - 0.0625 * part[t]


def pack_tiles(X, C, G, nw):
    rest = C[...]
    packed = None
    for _ in range(3):
        term = rest.astype(jnp.bfloat16)
        rest = rest - term.astype(f32)
        product = jnp.dot(X[...], term, preferred_element_type=f32)
        packed = product if packed is None else packed + product
    for d in range(nw):
        G[d] = packed[24 * d : 24 * d + CAP, :]


def kernel(
    nw, nn, l_ref, v_ref, route_ref, O, out_ref,
    F, M, V, S, Z, ys, yr, ys2, yr2, cr, H, Q, T, C, X, G,
    lsem, vsem, ssem, rsem, tsem, usem,
):
    w, n = lax.axis_index("wide"), lax.axis_index("narrow")
    left, right = lax.rem(w + nw - 1, nw), lax.rem(w + 1, nw)
    down, up = lax.rem(n + nn - 1, nn), lax.rem(n + 1, nn)
    lane = lanes_iota()

    loads = [
        pltpu.make_async_copy(
            l_ref.at[:, :, c * 128 : c * 128 + 128], F.at[3:35, c, 8:72, :], lsem.at[c]
        )
        for c in range(4)
    ]
    speeds = [
        pltpu.make_async_copy(v_ref.at[:, a:b], V.at[:, a:b], vsem.at[i])
        for i, (a, b) in enumerate(((3, 16), (0, 3), (16, 32)))
    ]
    for copy in loads + speeds:
        copy.start()

    barrier = pltpu.get_barrier_semaphore()

    def greet(a, b):
        pl.semaphore_signal(
            barrier, inc=1, device_id={"wide": a, "narrow": b}, device_id_type=pl.DeviceIdType.MESH
        )

    def greet_wide(i, _):
        greet(lax.rem(w + i, nw), n)
        return 0

    lax.fori_loop(1, nw, greet_wide, 0)
    for a in (left, w, right):
        for b in (down, up):
            greet(a, b)
    pl.semaphore_wait(barrier, nw - 1 + 6)

    def send(src, dst, k, a, b):
        return pltpu.make_async_remote_copy(
            src_ref=src,
            dst_ref=dst,
            send_sem=ssem.at[k],
            recv_sem=rsem.at[k],
            device_id={"wide": a, "narrow": b},
            device_id_type=pl.DeviceIdType.MESH,
        )

    def sides(field, sent, got, k):
        return (
            [
                send(field.at[3:6, :, 8:72, :], field.at[35:38, :, 8:72, :], k, left, n),
                send(field.at[32:35, :, 8:72, :], field.at[0:3, :, 8:72, :], k + 1, right, n),
            ],
            [
                send(sent.at[0], got.at[1], k + 2, w, down),
                send(sent.at[1], got.at[0], k + 3, w, up),
            ],
        )

    first_x, first_y = sides(F, ys, yr, 0)
    second_x, second_y = sides(M, ys2, yr2, 4)
    corners = [
        send(ys2.at[0, :, 0:16, :], cr.at[1, 1], 8, left, down),
        send(ys2.at[1, :, 0:16, :], cr.at[1, 0], 9, left, up),
        send(ys2.at[0, :, 80:96, :], cr.at[0, 1], 10, right, down),
        send(ys2.at[1, :, 80:96, :], cr.at[0, 0], 11, right, up),
    ]

    for copy in loads:
        copy.wait()
    for copy in first_x:
        copy.start()
    pack_rows(F, ys)
    for copy in first_y:
        copy.start()
    place_tiles(route_ref, X, nw)
    def inner(start):
        return lambda i: (3 + (i + start) // 2, pl.multiple_of(16 + 16 * lax.rem(i + start, 2), 16))

    def rims(i):
        return i // 2, pl.multiple_of(48 * lax.rem(i, 2), 16)

    def ends(i):
        k = i // 2
        return k + 26 * (k // 3), pl.multiple_of(16 + 16 * lax.rem(i, 2), 16)

    speeds[0].wait()
    advect_groups(26, inner(0), F, V, M, Z)
    speeds[1].wait()
    speeds[2].wait()
    for copy in first_x + first_y:
        copy.wait()
    unpack_rows(F, yr)
    advect_groups(64, rims, F, V, M, Z)
    pack_rows(M, ys2)
    for copy in second_y + corners:
        copy.start()
    advect_groups(12, ends, F, V, M, Z)
    for copy in second_x:
        copy.start()
    advect_groups(26, inner(26), F, V, M, Z)
    for copy in second_x + second_y + corners:
        copy.wait()
    unpack_rows(M, yr2)
    for xs in range(2):
        for ysd in range(2):
            for j in range(3):
                row = (5, 72)[ysd]
                at = (7, 0)[xs] + 3 * j
                for c in range(4):
                    M[35 * xs + j, c, row : row + 3, :] = cr[xs, ysd, c, at : at + 3, :]

    def sweep(src, dst, row0, first, count, planes):
        def body(i, _):
            x = planes(i)
            for b in range(9):
                r = row0 + 8 * b
                new = sweep_block(x, r, src, dst, S, lane, True if first else None)
                for c in range(4):
                    dst[x, c, pl.ds(r, 8), :] = new[c]
            return 0

        lax.fori_loop(0, count, body, 0)

    def two(start, count):
        return 2 * count, lambda i: start + lax.rem(i, count) + 16 * (i // count)

    def last_sweep(q):
        def body(i, _):
            tile, pair = i // 2, lax.rem(i, 2)
            x0 = 4 * q + 2 * pair + 16 * tile
            for b in range(8):
                both = []
                for half in range(2):
                    new = sweep_block(x0 + half + 3, 8 + 8 * b, M, None, S, lane)
                    for c in range(4):
                        O[x0 + half, c, 8 * b : 8 * b + 8, :] = new[c]
                    both.append([v * lax.rsqrt(v * v + 1.0) for v in new])
                for c in range(4):
                    H[c, 8 * b : 8 * b + 8, :] = both[0][c] + both[1][c]
            for yt in range(4):
                for c in range(4):
                    Q[c, pl.ds(pair * 64 + tile * 4 + yt, 8, stride=8), :] = (
                        H[c, pl.ds(16 * yt, 8, stride=2), :]
                        + H[c, pl.ds(16 * yt + 1, 8, stride=2), :]
                    )
            return 0

        lax.fori_loop(0, 4, body, 0)

    steps = [
        (dx, (r + i) % 4, r // 4)
        for r in range(8)
        for i, dx in enumerate((1, 3, 2, 0))
        if (dx, (r + i) % 4, r // 4) != (0, 0, 0)
    ]

    def tile_copy(q, j):
        dx, dz, dc = steps[j]
        z, x, core = w // 8, lax.rem(w // 2, 4), lax.rem(w, 2)
        to = lax.rem(z + dz, nw // 8) * 8 + lax.rem(x + dx, 4) * 2 + lax.rem(core + dc, 2)
        return pltpu.make_async_remote_copy(
            src_ref=G.at[q, to],
            dst_ref=out_ref.at[q, w],
            send_sem=tsem.at[q, j],
            recv_sem=usem.at[q, j],
            device_id={"wide": to},
            device_id_type=pl.DeviceIdType.MESH,
        )

    copies = []
    for q in range(4):
        if q == 0:
            sweep(M, F, 6, True, *two(1, 8))
            sweep(F, M, 7, False, *two(2, 6))
        elif q < 3:
            sweep(M, F, 6, True, *two(4 * q + 5, 4))
            sweep(F, M, 7, False, *two(4 * q + 4, 4))
        else:
            sweep(M, F, 6, True, 4, lambda i: i + 33)
            sweep(F, M, 7, False, 6, lambda i: i + 16 + 14 * ((i + 2) // 4))
        last_sweep(q)
        gather_tiles(Q, T, C)
        pack_tiles(X, C, G.at[q], nw)
        here = [tile_copy(q, j) for j in range(nw - 1)]
        out_ref[q, w] = G[q, w]
        for copy in here:
            copy.start()
        copies += here

    for copy in copies:
        copy.wait()


def finish_kernel(nw, field_ref, slots_ref, surf_ref, out_ref, W, osem, psem):
    puts = [
        pltpu.make_async_copy(field_ref.at[:, c], surf_ref.at[:, :, 128 * c : 128 * c + 128], osem.at[c])
        for c in range(4)
    ]
    for copy in puts:
        copy.start()
    for q in range(4):
        for d in range(nw):
            W[q, CAP * d : CAP * d + CAP, :] = slots_ref[q, d]
        puts.append(
            pltpu.make_async_copy(W.at[q], out_ref.at[:, 128 * q : 128 * q + 128], psem.at[q])
        )
        puts[-1].start()
    for copy in puts:
        copy.wait()


def solution(mesh):
    nw, nn = mesh.shape["wide"], mesh.shape["narrow"]
    rows = pltpu.VMEM((2, 4, 96, 128), f32)
    dma = pltpu.SemaphoreType.DMA
    hbm = pl.BlockSpec(memory_space=pltpu.HBM)
    vmem = pl.BlockSpec(memory_space=pltpu.VMEM)
    call = pl.pallas_call(
        functools.partial(kernel, nw, nn),
        out_shape=(
            pltpu.VMEM((CX, 4, CY, 128), f32),
            pltpu.VMEM((4, nw, CAP, 128), f32),
        ),
        in_specs=[hbm, hbm, vmem],
        out_specs=(vmem, vmem),
        scratch_shapes=[
            pltpu.VMEM(FIELD, f32),
            pltpu.VMEM(FIELD, f32),
            pltpu.VMEM((3, CX, CY, CZ), jnp.bfloat16),
            pltpu.VMEM(FIELD, f32),
            pltpu.VMEM((2, 2, 4, 16, 128), f32),
            rows,
            rows,
            rows,
            rows,
            pltpu.VMEM((2, 2, 4, 16, 128), f32),
            pltpu.VMEM((4, CY, 128), f32),
            pltpu.VMEM((4, 128, 128), f32),
            pltpu.VMEM((512, 128), f32),
            pltpu.VMEM((256, 128), f32),
            pltpu.VMEM((nw * 24, 256), jnp.bfloat16),
            pltpu.VMEM((4, nw, CAP, 128), f32),
            dma((4,)),
            dma((3,)),
            dma((12,)),
            dma((12,)),
            dma((4, nw)),
            dma((4, nw)),
        ],
        compiler_params=pltpu.CompilerParams(
            collective_id=0, has_side_effects=True, vmem_limit_bytes=57 << 20
        ),
        name="level_set_step",
    )
    finish = pl.pallas_call(
        functools.partial(finish_kernel, nw),
        out_shape=(
            jax.ShapeDtypeStruct((CX, CY, CZ), f32),
            jax.ShapeDtypeStruct((nw * CAP, 512), f32),
        ),
        in_specs=[vmem, vmem],
        out_specs=(hbm, hbm),
        scratch_shapes=[pltpu.VMEM((4, nw * CAP, 128), f32), dma((4,)), dma((4,))],
        compiler_params=pltpu.CompilerParams(vmem_limit_bytes=16 << 20),
        name="finish",
    )

    def on_device(level_set, velocity, box_owner):
        surface, slots = finish(*call(level_set, velocity, box_owner.reshape(1, -1)))
        return surface, slots.reshape(1, 1, nw * CAP, 512)

    return jax.shard_map(
        on_device,
        mesh=mesh,
        in_specs=(
            P("wide", "narrow", None),
            P(None, "wide", "narrow", None),
            P("wide", "narrow", None, None),
        ),
        out_specs=(P("wide", "narrow", None), P("wide", "narrow", None, None)),
        check_vma=False,
    )
```

```python
import functools

import jax
import jax.numpy as jnp
from jax import lax
from jax.experimental import pallas as pl
from jax.experimental.pallas import tpu as pltpu
from jax.sharding import PartitionSpec as P

f32 = jnp.float32
EPS = 0.75e-6
CX, CY, CZ = 32, 64, 512
CAP = 20
FIELD = (38, 4, 80, 128)


def lanes_iota():
    return lax.broadcasted_iota(jnp.int32, (8, 128), 1)


def lane_from(prev, cur, k, lane):
    return pltpu.roll(jnp.where(lane >= 128 - k, prev, cur), k, 1)


def lane_to(cur, nxt, k, lane):
    return pltpu.roll(jnp.where(lane < k, nxt, cur), 128 - k, 1)


def corr(E1, E2, E3, E4):
    E2s = 0.75 * E2
    E3s = 0.75 * E3
    t1 = E2 - E1
    S1 = t1 * t1 + (E2s * (t1 + E2) + EPS)
    t2 = E3 - E2
    S2 = t2 * t2 + (E2s * E3 + EPS)
    t3 = E3 - E4
    S3 = t3 * t3 + (E3s * (t3 + E3) + EPS)
    r1 = 1.0 / S1
    r2 = 1.0 / S2
    r3 = 1.0 / S3
    w1 = r1 * r1
    w2 = (6.0 * r2) * r2
    w3 = (3.0 * r3) * r3
    return (E2 + (E3 + E3)) - ((w1 + w1) * (t2 - t1) - w3 * (t2 + t3)) / (w1 + w2 + w3)


def upwind(u, dm, dp, qm2, qm1, q0, qp1, qp2):
    p = u > 0
    V3 = jnp.where(p, dm, dp)
    E1 = jnp.where(p, qm2, qp2)
    E2 = jnp.where(p, qm1, qp1)
    E4 = jnp.where(p, qp1, qm1)
    return u * V3 + (jnp.abs(u) * (1.0 / 6.0)) * corr(E1, E2, q0, E4)


def differences(fs):
    d = [fs[i + 1] - fs[i] for i in range(6)]
    q = [d[i + 1] - d[i] for i in range(5)]
    return (d[2], d[3], *q)


def third_differences(x, row, F, Z, Y):
    lane = lanes_iota()
    for h in range(2):
        fc = [F[x + 3, c, pl.ds(row + 8 * h + 8, 8), :] for c in range(4)]
        for c in range(4):
            if c > 0:
                fm = lane_from(fc[c - 1], fc[c], 1, lane)
            else:
                fm = jnp.where(lane == 0, fc[0], pltpu.roll(fc[0], 1, 1))
            if c < 3:
                fp = lane_to(fc[c], fc[c + 1], 1, lane)
            else:
                fp = jnp.where(lane == 127, fc[3], pltpu.roll(fc[3], 127, 1))
            dm = fc[c] - fm
            Z[0, c, 8 * h : 8 * h + 8, :] = (fp - fc[c]) - dm
            Z[1, c, 8 * h : 8 * h + 8, :] = dm
    for c in range(4):
        for b in range(3):
            at = row + 6 + 8 * b
            f = F[x + 3, c, pl.ds(at, 8), :]
            Y[c, 8 * b : 8 * b + 8, :] = (F[x + 3, c, pl.ds(at + 1, 8), :] - f) - (
                f - F[x + 3, c, pl.ds(at - 1, 8), :]
            )


def advect_group(x, row, F, V, M, Z, Y):
    lane = lanes_iota()
    zero = jnp.zeros((8, 128), f32)
    for h in range(2):
        r = row + 8 * h + 8
        q = [zero, *(Z[0, c, 8 * h : 8 * h + 8, :] for c in range(4)), zero]
        for c in range(4):
            f = F[x + 3, c, pl.ds(r, 8), :]
            u = V[:, x, pl.ds(row, 16), c * 128 : c * 128 + 128][:, 8 * h : 8 * h + 8].astype(f32)
            fx = [f if k == 3 else F[x + k, c, pl.ds(r, 8), :] for k in range(7)]
            acc = upwind(u[0], *differences(fx))
            acc = acc + upwind(
                u[1],
                f - F[x + 3, c, pl.ds(r - 1, 8), :],
                F[x + 3, c, pl.ds(r + 1, 8), :] - f,
                *(Y[c, 8 * h + k : 8 * h + k + 8, :] for k in range(5)),
            )
            dm = Z[1, c, 8 * h : 8 * h + 8, :]
            qp, qc, qn = q[c : c + 3]
            acc = acc + upwind(
                u[2],
                dm,
                dm + qc,
                lane_from(qp, qc, 2, lane),
                lane_from(qp, qc, 1, lane),
                qc,
                lane_to(qc, qn, 1, lane),
                lane_to(qc, qn, 2, lane),
            )
            M[x + 3, c, pl.ds(r, 8), :] = f - acc


def advect_groups(count, place, F, V, M, Z, Y):
    third_differences(*place(0), F, Z.at[0], Y.at[0])

    def body(i, _):
        advect_group(*place(i), F, V, M, Z.at[lax.rem(i, 2)], Y.at[lax.rem(i, 2)])
        nxt = lax.rem(i + 1, 2)
        third_differences(*place(lax.rem(i + 1, count)), F, Z.at[nxt], Y.at[nxt])
        return 0

    lax.fori_loop(0, count, body, 0)


def pack_rows(field, buf):
    def body(k, _):
        for j in range(8):
            for c in range(4):
                for s, row in ((0, 8), (1, 69)):
                    buf[s, c, pl.ds(k * 24 + 3 * j, 3), :] = field[k * 8 + j + 3, c, row : row + 3, :]
        return 0

    lax.fori_loop(0, 4, body, 0)


def unpack_rows(field, buf):
    def body(k, _):
        for j in range(8):
            for c in range(4):
                for s, row in ((0, 5), (1, 72)):
                    field[k * 8 + j + 3, c, row : row + 3, :] = buf[s, c, pl.ds(k * 24 + 3 * j, 3), :]
        return 0

    lax.fori_loop(0, 4, body, 0)


def sweep_block(x, r, src, dst, S, lane, moved=None):
    fc = [src[x, c, pl.ds(r, 8), :] for c in range(4)]
    new = []
    for c in range(4):
        cur = fc[c]
        if moved is None:
            s = S[x, c, pl.ds(r, 8), :]
        else:
            s = (0.3 * cur) * lax.rsqrt(cur * cur + 1.0)
            S[x, c, pl.ds(r, 8), :] = s
        sg = jnp.where(s > 0, 1.0, -1.0)
        sc = sg * cur

        def term(lo, hi):
            e = sc - jnp.minimum(jnp.minimum(sg * lo, sg * hi), sc)
            return e * e

        G = term(src[x - 1, c, pl.ds(r, 8), :], src[x + 1, c, pl.ds(r, 8), :])
        G = G + term(src[x, c, pl.ds(r - 1, 8), :], src[x, c, pl.ds(r + 1, 8), :])
        if c > 0:
            lo = lane_from(fc[c - 1], cur, 1, lane)
        else:
            lo = jnp.where(lane == 0, cur, pltpu.roll(cur, 1, 1))
        if c < 3:
            hi = lane_to(cur, fc[c + 1], 1, lane)
        else:
            hi = jnp.where(lane == 127, cur, pltpu.roll(cur, 127, 1))
        G = G + term(lo, hi)
        root = G * lax.rsqrt(jnp.maximum(G, 1e-37))
        new.append(cur - s * (root - 1.0))
    return new


def iota(shape, dim):
    return lax.broadcasted_iota(jnp.int32, shape, dim)


def place_tiles(route_ref, X, nw):
    tiles = route_ref.shape[1]
    route = route_ref[...]
    matches = (route == iota((nw, tiles), 0)).astype(f32)
    before = (iota((tiles, tiles), 0) < iota((tiles, tiles), 1)).astype(f32)
    earlier = jnp.dot(
        matches.astype(jnp.bfloat16), before.astype(jnp.bfloat16), preferred_element_type=f32
    )
    position = jnp.sum(earlier * matches, axis=0, keepdims=True).astype(jnp.int32)
    target = route * 24 + position
    X[...] = (iota((nw * 24, tiles), 0) == target).astype(f32).astype(jnp.bfloat16)


def gather_tiles(Q, T, C):
    for c in range(4):
        T[c * 128 : c * 128 + 128, :] = Q[c].T
    lane = lanes_iota()
    for zv in range(4):
        part = [
            T[pl.ds(128 * zv + 2 * z, 8, stride=16), :] + T[pl.ds(128 * zv + 2 * z + 1, 8, stride=16), :]
            for z in range(8)
        ]
        for s in (1, 2, 4):
            bit = (lane & s) > 0
            for z in range(8):
                if z & s == 0:
                    a, b = part[z], part[z | s]
                    part[z] = jnp.where(bit, pltpu.roll(b, s, 1), a)
                    part[z | s] = jnp.where(bit, b, pltpu.roll(a, 128 - s, 1))
        for t in range(8):
            C[32 * t + 8 * zv : 32 * t + 8 * zv + 8, :] = 0.5 - 0.0625 * part[t]


def pack_tiles(X, C, G, nw):
    rest = C[...]
    packed = None
    for _ in range(3):
        term = rest.astype(jnp.bfloat16)
        rest = rest - term.astype(f32)
        product = jnp.dot(X[...], term, preferred_element_type=f32)
        packed = product if packed is None else packed + product
    for d in range(nw):
        G[d] = packed[24 * d : 24 * d + CAP, :]


def kernel(
    nw, nn, l_ref, v_ref, route_ref, O, out_ref,
    F, M, V, S, Z, Y, ys, yr, ys2, yr2, cr, H, Q, T, C, X, G,
    lsem, vsem, ssem, rsem, tsem, usem,
):
    w, n = lax.axis_index("wide"), lax.axis_index("narrow")
    left, right = lax.rem(w + nw - 1, nw), lax.rem(w + 1, nw)
    down, up = lax.rem(n + nn - 1, nn), lax.rem(n + 1, nn)
    lane = lanes_iota()

    loads = [
        pltpu.make_async_copy(
            l_ref.at[:, :, c * 128 : c * 128 + 128], F.at[3:35, c, 8:72, :], lsem.at[c]
        )
        for c in range(4)
    ]
    speeds = [
        pltpu.make_async_copy(v_ref.at[:, a:b], V.at[:, a:b], vsem.at[i])
        for i, (a, b) in enumerate(((3, 16), (0, 3), (16, 32)))
    ]
    for copy in loads + speeds:
        copy.start()

    barrier = pltpu.get_barrier_semaphore()

    def greet(a, b):
        pl.semaphore_signal(
            barrier, inc=1, device_id={"wide": a, "narrow": b}, device_id_type=pl.DeviceIdType.MESH
        )

    def greet_wide(i, _):
        greet(lax.rem(w + i, nw), n)
        return 0

    lax.fori_loop(1, nw, greet_wide, 0)
    for a in (left, w, right):
        for b in (down, up):
            greet(a, b)
    pl.semaphore_wait(barrier, nw - 1 + 6)

    def send(src, dst, k, a, b):
        return pltpu.make_async_remote_copy(
            src_ref=src,
            dst_ref=dst,
            send_sem=ssem.at[k],
            recv_sem=rsem.at[k],
            device_id={"wide": a, "narrow": b},
            device_id_type=pl.DeviceIdType.MESH,
        )

    def sides(field, sent, got, k):
        return (
            [
                send(field.at[3:6, :, 8:72, :], field.at[35:38, :, 8:72, :], k, left, n),
                send(field.at[32:35, :, 8:72, :], field.at[0:3, :, 8:72, :], k + 1, right, n),
            ],
            [
                send(sent.at[0], got.at[1], k + 2, w, down),
                send(sent.at[1], got.at[0], k + 3, w, up),
            ],
        )

    first_x, first_y = sides(F, ys, yr, 0)
    second_x, second_y = sides(M, ys2, yr2, 4)
    corners = [
        send(ys2.at[0, :, 0:16, :], cr.at[1, 1], 8, left, down),
        send(ys2.at[1, :, 0:16, :], cr.at[1, 0], 9, left, up),
        send(ys2.at[0, :, 80:96, :], cr.at[0, 1], 10, right, down),
        send(ys2.at[1, :, 80:96, :], cr.at[0, 0], 11, right, up),
    ]

    for copy in loads:
        copy.wait()
    for copy in first_x:
        copy.start()
    pack_rows(F, ys)
    for copy in first_y:
        copy.start()
    place_tiles(route_ref, X, nw)
    def inner(start):
        return lambda i: (3 + (i + start) // 2, pl.multiple_of(16 + 16 * lax.rem(i + start, 2), 16))

    def rims(i):
        return i // 2, pl.multiple_of(48 * lax.rem(i, 2), 16)

    def ends(i):
        k = i // 2
        return k + 26 * (k // 3), pl.multiple_of(16 + 16 * lax.rem(i, 2), 16)

    speeds[0].wait()
    advect_groups(26, inner(0), F, V, M, Z, Y)
    speeds[1].wait()
    speeds[2].wait()
    for copy in first_x + first_y:
        copy.wait()
    unpack_rows(F, yr)
    advect_groups(64, rims, F, V, M, Z, Y)
    pack_rows(M, ys2)
    for copy in second_y + corners:
        copy.start()
    advect_groups(12, ends, F, V, M, Z, Y)
    for copy in second_x:
        copy.start()
    advect_groups(26, inner(26), F, V, M, Z, Y)
    for copy in second_x + second_y + corners:
        copy.wait()
    unpack_rows(M, yr2)
    for xs in range(2):
        for ysd in range(2):
            for j in range(3):
                row = (5, 72)[ysd]
                at = (7, 0)[xs] + 3 * j
                for c in range(4):
                    M[35 * xs + j, c, row : row + 3, :] = cr[xs, ysd, c, at : at + 3, :]

    def sweep(src, dst, row0, first, count, planes):
        def body(i, _):
            x = planes(i)
            for b in range(9):
                r = row0 + 8 * b
                new = sweep_block(x, r, src, dst, S, lane, True if first else None)
                for c in range(4):
                    dst[x, c, pl.ds(r, 8), :] = new[c]
            return 0

        lax.fori_loop(0, count, body, 0)

    def two(start, count):
        return 2 * count, lambda i: start + lax.rem(i, count) + 16 * (i // count)

    def last_sweep(q):
        def body(i, _):
            tile, pair = i // 2, lax.rem(i, 2)
            x0 = 4 * q + 2 * pair + 16 * tile
            for b in range(8):
                both = []
                for half in range(2):
                    new = sweep_block(x0 + half + 3, 8 + 8 * b, M, None, S, lane)
                    for c in range(4):
                        O[x0 + half, c, 8 * b : 8 * b + 8, :] = new[c]
                    both.append([v * lax.rsqrt(v * v + 1.0) for v in new])
                for c in range(4):
                    H[c, 8 * b : 8 * b + 8, :] = both[0][c] + both[1][c]
            for yt in range(4):
                for c in range(4):
                    Q[c, pl.ds(pair * 64 + tile * 4 + yt, 8, stride=8), :] = (
                        H[c, pl.ds(16 * yt, 8, stride=2), :]
                        + H[c, pl.ds(16 * yt + 1, 8, stride=2), :]
                    )
            return 0

        lax.fori_loop(0, 4, body, 0)

    steps = [
        (dx, (r + i) % 4, r // 4)
        for r in range(8)
        for i, dx in enumerate((1, 3, 2, 0))
        if (dx, (r + i) % 4, r // 4) != (0, 0, 0)
    ]

    def tile_copy(q, j):
        dx, dz, dc = steps[j]
        z, x, core = w // 8, lax.rem(w // 2, 4), lax.rem(w, 2)
        to = lax.rem(z + dz, nw // 8) * 8 + lax.rem(x + dx, 4) * 2 + lax.rem(core + dc, 2)
        return pltpu.make_async_remote_copy(
            src_ref=G.at[q, to],
            dst_ref=out_ref.at[q, w],
            send_sem=tsem.at[q, j],
            recv_sem=usem.at[q, j],
            device_id={"wide": to},
            device_id_type=pl.DeviceIdType.MESH,
        )

    copies = []
    for q in range(4):
        if q == 0:
            sweep(M, F, 6, True, *two(1, 8))
            sweep(F, M, 7, False, *two(2, 6))
        elif q < 3:
            sweep(M, F, 6, True, *two(4 * q + 5, 4))
            sweep(F, M, 7, False, *two(4 * q + 4, 4))
        else:
            sweep(M, F, 6, True, 4, lambda i: i + 33)
            sweep(F, M, 7, False, 6, lambda i: i + 16 + 14 * ((i + 2) // 4))
        last_sweep(q)
        gather_tiles(Q, T, C)
        pack_tiles(X, C, G.at[q], nw)
        here = [tile_copy(q, j) for j in range(nw - 1)]
        out_ref[q, w] = G[q, w]
        for copy in here:
            copy.start()
        copies += here

    for copy in copies:
        copy.wait()


def finish_kernel(nw, field_ref, slots_ref, surf_ref, out_ref, W, osem, psem):
    puts = [
        pltpu.make_async_copy(field_ref.at[:, c], surf_ref.at[:, :, 128 * c : 128 * c + 128], osem.at[c])
        for c in range(4)
    ]
    for copy in puts:
        copy.start()
    for q in range(4):
        for d in range(nw):
            W[q, CAP * d : CAP * d + CAP, :] = slots_ref[q, d]
        puts.append(
            pltpu.make_async_copy(W.at[q], out_ref.at[:, 128 * q : 128 * q + 128], psem.at[q])
        )
        puts[-1].start()
    for copy in puts:
        copy.wait()


def solution(mesh):
    nw, nn = mesh.shape["wide"], mesh.shape["narrow"]
    rows = pltpu.VMEM((2, 4, 96, 128), f32)
    dma = pltpu.SemaphoreType.DMA
    hbm = pl.BlockSpec(memory_space=pltpu.HBM)
    vmem = pl.BlockSpec(memory_space=pltpu.VMEM)
    call = pl.pallas_call(
        functools.partial(kernel, nw, nn),
        out_shape=(
            pltpu.VMEM((CX, 4, CY, 128), f32),
            pltpu.VMEM((4, nw, CAP, 128), f32),
        ),
        in_specs=[hbm, hbm, vmem],
        out_specs=(vmem, vmem),
        scratch_shapes=[
            pltpu.VMEM(FIELD, f32),
            pltpu.VMEM(FIELD, f32),
            pltpu.VMEM((3, CX, CY, CZ), jnp.bfloat16),
            pltpu.VMEM(FIELD, f32),
            pltpu.VMEM((2, 2, 4, 16, 128), f32),
            pltpu.VMEM((2, 4, 24, 128), f32),
            rows,
            rows,
            rows,
            rows,
            pltpu.VMEM((2, 2, 4, 16, 128), f32),
            pltpu.VMEM((4, CY, 128), f32),
            pltpu.VMEM((4, 128, 128), f32),
            pltpu.VMEM((512, 128), f32),
            pltpu.VMEM((256, 128), f32),
            pltpu.VMEM((nw * 24, 256), jnp.bfloat16),
            pltpu.VMEM((4, nw, CAP, 128), f32),
            dma((4,)),
            dma((3,)),
            dma((12,)),
            dma((12,)),
            dma((4, nw)),
            dma((4, nw)),
        ],
        compiler_params=pltpu.CompilerParams(
            collective_id=0, has_side_effects=True, vmem_limit_bytes=57 << 20
        ),
        name="level_set_step",
    )
    finish = pl.pallas_call(
        functools.partial(finish_kernel, nw),
        out_shape=(
            jax.ShapeDtypeStruct((CX, CY, CZ), f32),
            jax.ShapeDtypeStruct((nw * CAP, 512), f32),
        ),
        in_specs=[vmem, vmem],
        out_specs=(hbm, hbm),
        scratch_shapes=[pltpu.VMEM((4, nw * CAP, 128), f32), dma((4,)), dma((4,))],
        compiler_params=pltpu.CompilerParams(vmem_limit_bytes=16 << 20),
        name="finish",
    )

    def on_device(level_set, velocity, box_owner):
        surface, slots = finish(*call(level_set, velocity, box_owner.reshape(1, -1)))
        return surface, slots.reshape(1, 1, nw * CAP, 512)

    return jax.shard_map(
        on_device,
        mesh=mesh,
        in_specs=(
            P("wide", "narrow", None),
            P(None, "wide", "narrow", None),
            P("wide", "narrow", None, None),
        ),
        out_specs=(P("wide", "narrow", None), P("wide", "narrow", None, None)),
        check_vma=False,
    )
```
